32 devices in a mesh: groups: 2 (over x), seq: 8 (over z, y), head: 2 (over core).
Axes of the slice: x: 2, y: 2, z: 4, core: 2. Of those that a mesh axis runs over, the one named last changes fastest.
Arguments:
- queries: bfloat16 [4096, 3584], P(('groups', 'seq'), 'head'), parts along dimension 0, may hold values from -30 to 30
- current_keys: bfloat16 [4096, 512], P(('groups', 'seq'), 'head'), parts along dimension 0, may hold values from -6 to 6
- current_values: bfloat16 [4096, 512], P(('groups', 'seq'), 'head'), parts along dimension 0, may hold values from -6 to 6
- stored_keys: bfloat16 [4096, 2, 512], P(('groups', 'seq'), None, 'head'), parts along dimension 0, may hold values from -22 to 22
- stored_values: bfloat16 [4096, 2, 512], P(('groups', 'seq'), None, 'head'), parts along dimension 0, may hold values from -6 to 6
- remap_table: int32 [3, 64], P(None, ('groups', 'seq')), parts along dimension 1, may hold values from 0 to 2047
- block_table: int32 [256], P('groups'), parts along dimension 0, may hold values from 0 to 15, as said below
Outputs:
- attended: bfloat16 [4096, 3584], P(('groups', 'seq'), 'head'), parts along dimension 0
- paged_keys: bfloat16 [4, 256, 2048], P('head', ('groups', 'seq')), parts along dimension 1
- paged_values: bfloat16 [4, 256, 2048], P('head', ('groups', 'seq')), parts along dimension 1
The draws below stay inside these ranges and needn't reach their ends.
There are 2 independent parts, one for each index of `groups`. The reference program is written for one: setup_inputs(seed, part) draws one part's arguments, and reference() takes and returns one part's arrays. A program takes and returns all parts, laid end to end along the dimension named above; each array names one. Nothing has to cross between parts.
Inputs may be any that keep to these rules, and one draw needn't show every extreme that they name: `block_table`: the entries of the blocks b that share b modulo 8 are a permutation of 0 to 15.
All inputs are finite; a program needn't handle non-finite values.
Results may differ from the reference program's by a relative error of at most 0.012.
The reference program's roundings to bfloat16 on the way count: a program that leaves them out, or rounds other values in their place, can miss the bound.
Values may be sent and summed in bfloat16 or wider, within the bound.
A program may use at most 128 MiB of HBM per device.

```python
import jax
import jax.numpy as jnp
from jax import lax

HQ = 28
KEY_VALUE_HEADS = 4
HEAD_SIZE = 128
PRIOR_SEGMENTS = 2
PAGE_TOKENS = 16
QBLK = 64
QUERY_PER_KEY = 7
SEGMENT_TOKENS = 2048
NQB = 32
SEGMENT_PAGES = 128
OWNERS = 8
PAGES_DEV = 16


def draw_queries(key, part):
    rotary_base = jnp.clip(jax.random.normal(jax.random.fold_in(key, 1), (SEGMENT_TOKENS, HQ * HEAD_SIZE), jnp.float32), -6.0, 6.0) * 2.2
    return rotary_base.astype(jnp.bfloat16)


def draw_stored_keys(key, part):
    rotary_base = jnp.clip(jax.random.normal(jax.random.fold_in(key, 2), (SEGMENT_TOKENS, PRIOR_SEGMENTS, KEY_VALUE_HEADS * HEAD_SIZE), jnp.float32), -6.0, 6.0)
    return rotary_base.astype(jnp.bfloat16)


def draw_block_table(key, part):
    holder_keys = jax.random.split(jax.random.fold_in(key, 5), OWNERS)
    orders = jax.vmap(lambda single: jax.random.permutation(single, PAGES_DEV))(holder_keys)
    return orders.T.reshape(-1).astype(jnp.int32)


def touch_ends(entries, own_key, smallest, top_value):
    spot = [jax.random.randint(jax.random.fold_in(own_key, axis), (), 0, length) for axis, length in enumerate(entries.shape)]
    main_axis = entries.shape.index(max(entries.shape))
    beside = spot[:main_axis] + [(spot[main_axis] + 1) % entries.shape[main_axis]] + spot[main_axis + 1:]
    return entries.at[tuple(spot)].set(smallest).at[tuple(beside)].set(top_value)


def block_levels(own_key, dims, cuts, least, top_value):
    def one(dim, shards_of):
        steps = jax.random.uniform(jax.random.fold_in(jax.random.fold_in(own_key, 6), dim), (shards_of,), jnp.float32, least / len(cuts), top_value / len(cuts))
        return jnp.repeat(jnp.exp(steps), dims[dim] // shards_of).reshape((-1,) + (1,) * (len(dims) - dim - 1))

    gain = one(*cuts[0])
    for cut in cuts[1:]:
        gain = gain * one(*cut)
    return gain


def scatter_about(stream_key, extent, spread, most, cuts=(), kind=jnp.bfloat16):
    loudness = block_levels(stream_key, extent, cuts, -0.22, 0.18) if cuts else 1.0
    values = jax.random.normal(stream_key, extent, jnp.float32) * spread * loudness
    return jnp.minimum(jnp.maximum(values, -most), most).astype(kind)


def setup_inputs(seed: int = 0, part: int = 0) -> dict:
    key_list = jax.random.split(jax.random.key(seed), 8)
    part_splits = jax.random.split(jax.random.fold_in(key_list[7], part), 8)
    queries = draw_queries(jax.random.fold_in(jax.random.fold_in(key_list[7], part), 71), part)
    current_keys = scatter_about(part_splits[1], (SEGMENT_TOKENS, KEY_VALUE_HEADS * HEAD_SIZE), 1.0, 6.0, ((0, 8), (1, 2)))
    current_values = scatter_about(part_splits[2], (SEGMENT_TOKENS, KEY_VALUE_HEADS * HEAD_SIZE), 1.0, 6.0, ((0, 8), (1, 2)))
    stored_keys = draw_stored_keys(jax.random.fold_in(jax.random.fold_in(key_list[7], part), 71), part)
    stored_values = scatter_about(part_splits[4], (SEGMENT_TOKENS, PRIOR_SEGMENTS, KEY_VALUE_HEADS * HEAD_SIZE), 1.0, 6.0, ((0, 8), (2, 2)))
    remap_table = touch_ends(jax.random.randint(part_splits[5], (3, NQB), 0, SEGMENT_TOKENS), jax.random.fold_in(part_splits[5], 1), 0, SEGMENT_TOKENS - 1).astype(jnp.int32)
    block_table = draw_block_table(jax.random.fold_in(jax.random.fold_in(key_list[7], part), 71), part)
    return dict(queries=queries, current_keys=current_keys, current_values=current_values, stored_keys=stored_keys, stored_values=stored_values, remap_table=remap_table, block_table=block_table)


rope_base = 1000000.0
masked_value = -1e30


def apply_rotary(values, token_positions):
    half_dim = values.shape[-1] // 2
    frequency = rope_base ** (-2.0 * jnp.arange(half_dim, dtype=jnp.float32) / values.shape[-1])
    angles = token_positions.astype(jnp.float32)[:, None] * frequency[None, :]
    cos_table = jnp.cos(angles)[:, None, :]
    sin_table = jnp.sin(angles)[:, None, :]
    first_half = values[..., :half_dim]
    second_half = values[..., half_dim:]
    return jnp.concatenate([first_half * cos_table - second_half * sin_table, second_half * cos_table + first_half * sin_table], -1)


def paged_layout(cache_portion, block_table):
    page_blocks = cache_portion.reshape(SEGMENT_PAGES, PAGE_TOKENS, KEY_VALUE_HEADS, HEAD_SIZE).transpose(2, 0, 1, 3).reshape(KEY_VALUE_HEADS, SEGMENT_PAGES, PAGE_TOKENS * HEAD_SIZE)
    block_index = jnp.arange(SEGMENT_PAGES, dtype=jnp.int32)
    target = (block_index % OWNERS) * PAGES_DEV + block_table
    return jnp.zeros_like(page_blocks).at[:, target].set(page_blocks)


def reference(queries, current_keys, current_values, stored_keys, stored_values, remap_table, block_table):
    token_index = jnp.arange(SEGMENT_TOKENS, dtype=jnp.int32)
    token_positions = jnp.repeat(remap_table, QBLK, axis=1) + (token_index % QBLK)[None, :]
    query_single_float = queries.astype(jnp.float32).reshape(SEGMENT_TOKENS, HQ, HEAD_SIZE)
    rotary_output = [apply_rotary(query_single_float, token_positions[segment_kind_index]).astype(jnp.bfloat16).reshape(SEGMENT_TOKENS, KEY_VALUE_HEADS, QUERY_PER_KEY, HEAD_SIZE) for segment_kind_index in range(3)]
    score_scale = HEAD_SIZE ** -0.5
    value_portions = [stored_values[:, segment_number, :] for segment_number in range(PRIOR_SEGMENTS)] + [current_values]
    joined_values = jnp.concatenate(value_portions, 0).reshape((PRIOR_SEGMENTS + 1) * SEGMENT_TOKENS, KEY_VALUE_HEADS, HEAD_SIZE).astype(jnp.float32)
    query_block = min(256, SEGMENT_TOKENS)

    def one_block(block_number):
        first_row = block_number * query_block
        score_parts = []
        for segment_number in range(PRIOR_SEGMENTS):
            chosen = rotary_output[2] if segment_number < PRIOR_SEGMENTS - 1 else rotary_output[1]
            query_rows = lax.dynamic_slice_in_dim(chosen, first_row, query_block, 0).astype(jnp.float32)
            key_row_list = stored_keys[:, segment_number, :].reshape(SEGMENT_TOKENS, KEY_VALUE_HEADS, HEAD_SIZE).astype(jnp.float32)
            score_parts.append(jnp.einsum("qgrd,kgd->grqk", query_rows, key_row_list) * score_scale)
        query_rows = lax.dynamic_slice_in_dim(rotary_output[0], first_row, query_block, 0).astype(jnp.float32)
        key_row_list = current_keys.reshape(SEGMENT_TOKENS, KEY_VALUE_HEADS, HEAD_SIZE).astype(jnp.float32)
        intra = jnp.einsum("qgrd,kgd->grqk", query_rows, key_row_list) * score_scale
        allowed = token_index[None, :] <= (first_row + jnp.arange(query_block, dtype=jnp.int32))[:, None]
        score_parts.append(jnp.where(allowed[None, None], intra, masked_value))
        scores = jnp.concatenate(score_parts, -1)
        weights = jnp.exp(scores - jnp.max(scores, -1, keepdims=True))
        denom = jnp.sum(weights, -1)
        rounded = weights.astype(jnp.bfloat16).astype(jnp.float32)
        summed = jnp.einsum("grqk,kgd->qgrd", rounded, joined_values)
        result = summed / denom.transpose(2, 0, 1)[..., None]
        return result.astype(jnp.bfloat16).reshape(query_block, HQ * HEAD_SIZE)

    attended = lax.map(one_block, jnp.arange(SEGMENT_TOKENS // query_block, dtype=jnp.int32)).reshape(SEGMENT_TOKENS, HQ * HEAD_SIZE)
    paged_keys = paged_layout(stored_keys[:, PRIOR_SEGMENTS - 1, :], block_table)
    paged_values = paged_layout(stored_values[:, PRIOR_SEGMENTS - 1, :], block_table)
    return (attended, paged_keys, paged_values)
```

```python
import functools
import math

import jax
import jax.numpy as jnp
from jax import lax
from jax.experimental import pallas as pl
from jax.experimental.pallas import tpu as pltpu
from jax.sharding import PartitionSpec as P

HEAD_SIZE = 128
PRIOR_SEGMENTS = 2
PAGE_TOKENS = 16
QBLK = 64
KINDS = PRIOR_SEGMENTS + 1
OWN_PART = PRIOR_SEGMENTS

rope_base = 1000000.0
masked_value = -1e30
MESH = pl.DeviceIdType.MESH
RIGHT, LEFT, ACROSS = 0, 1, 2


def kernel(
    n, kv_local, per_group, q_ref, cos_ref, sin_ref, kv_hbm, out_ref, raw_ref,
    held, turned, top, denom, total, own_sem, send_sem, recv_sem,
):
    me = lax.axis_index("seq")
    partner = me + 1 - 2 * (me % 2)
    tokens = q_ref.shape[0]
    heads = kv_local * per_group
    scale = HEAD_SIZE ** -0.5 * math.log2(math.e)
    has_right = me + 2 < n
    has_left = me - 2 >= 0

    own = pltpu.make_async_copy(kv_hbm, held.at[me], own_sem)
    own.start()
    barrier = pltpu.get_barrier_semaphore()
    pl.semaphore_signal(barrier, inc=1, device_id={"seq": partner}, device_id_type=MESH)

    @pl.when(has_right)
    def _():
        pl.semaphore_signal(barrier, inc=1, device_id={"seq": me + 2}, device_id_type=MESH)

    @pl.when(has_left)
    def _():
        pl.semaphore_signal(barrier, inc=1, device_id={"seq": me - 2}, device_id_type=MESH)

    expected = 1 + has_right.astype(jnp.int32) + has_left.astype(jnp.int32)
    pl.semaphore_wait(barrier, expected)
    own.wait()

    def remote(way, j, part):
        target = (me + 2, me - 2, partner)[way]
        return pltpu.make_async_remote_copy(
            src_ref=held.at[j, part],
            dst_ref=held.at[j, part],
            send_sem=send_sem.at[way, j, part],
            recv_sem=recv_sem.at[j, part],
            device_id={"seq": target},
            device_id_type=MESH,
        )

    def goes(way, j, part):
        mine = (j % 2) == (me % 2)
        stored = part < PRIOR_SEGMENTS
        if way == RIGHT:
            return mine & (j <= me) & has_right
        if way == LEFT:
            return mine & (j >= me) & stored & has_left
        return mine & (stored | (j <= partner))

    def forward(j, part):
        for way in (ACROSS, RIGHT, LEFT):

            @pl.when(goes(way, j, part))
            def _():
                remote(way, j, part).start()

    for part in range(KINDS):
        forward(me, part)

    def turn(part, carry):
        cos = cos_ref[part]
        sin = sin_ref[part]
        for h in range(heads):
            x = q_ref[:, h * HEAD_SIZE : (h + 1) * HEAD_SIZE].astype(jnp.float32)
            y = x * cos + pltpu.roll(x, HEAD_SIZE // 2, 1) * sin
            turned[part, h] = y.astype(jnp.bfloat16)
        return carry

    lax.fori_loop(0, KINDS, turn, 0)
    top[...] = jnp.full(top.shape, masked_value, jnp.float32)
    denom[...] = jnp.zeros(denom.shape, jnp.float32)
    total[...] = jnp.zeros(total.shape, jnp.float32)

    def absorb(j, part, causal):
        for g in range(kv_local):
            columns = slice(g * HEAD_SIZE, (g + 1) * HEAD_SIZE)
            keys = held[j, part, 0, :, columns]
            values = held[j, part, 1, :, columns].T
            for r in range(per_group):
                h = g * per_group + r
                scores = lax.dot_general(
                    keys, turned[part, h], (((1,), (1,)), ((), ())),
                    preferred_element_type=jnp.float32,
                )
                if causal:
                    key_index = lax.broadcasted_iota(jnp.int32, scores.shape, 0)
                    row_index = lax.broadcasted_iota(jnp.int32, scores.shape, 1)
                    scores = jnp.where(key_index <= row_index, scores, masked_value)
                old = top[h]
                new = jnp.maximum(old, jnp.max(scores, 0, keepdims=True))
                factor = jnp.exp2((old - new) * scale)
                weights = jnp.exp2((scores - new) * scale)
                top[h] = new
                denom[h] = denom[h] * factor + jnp.sum(weights, 0, keepdims=True)
                total[h] = total[h] * factor + jnp.dot(
                    values, weights.astype(jnp.bfloat16), preferred_element_type=jnp.float32
                )

    def own_step(part, carry):
        absorb(me, part, False)
        return carry

    lax.fori_loop(0, PRIOR_SEGMENTS, own_step, 0)
    absorb(me, OWN_PART, True)

    def round_step(step, carry):
        distance = step // (4 * KINDS) + 1
        part = (step // 4) % KINDS
        kind = step % 4
        near = distance - kind // 2
        start = jnp.where(kind < 2, me, partner)
        sign = 1 - 2 * (kind % 2)
        j = start - sign * 2 * near
        stored = part < PRIOR_SEGMENTS
        wanted = (j >= 0) & (j < n) & (stored | (j <= me)) & ((near > 0) | (kind % 2 == 0))

        @pl.when(wanted)
        def _():
            remote(RIGHT, j, part).wait_recv()
            forward(j, part)
            absorb(j, part, False)

        return carry

    lax.fori_loop(0, (n // 2) * 4 * KINDS, round_step, 0)

    rounds = tokens // PAGE_TOKENS // n
    last = PRIOR_SEGMENTS - 1

    def page_step(j, carry):
        for r in range(rounds):
            rows = pl.ds(pl.multiple_of((r * n + me) * PAGE_TOKENS, PAGE_TOKENS), PAGE_TOKENS)
            for which in range(2):
                raw_ref[which, j * rounds + r] = held[j, last, which, rows, :]
        return carry

    lax.fori_loop(0, n, page_step, 0)

    for h in range(heads):
        finished = total[h] / denom[h]
        out_ref[:, h * HEAD_SIZE : (h + 1) * HEAD_SIZE] = finished.T.astype(out_ref.dtype)

    def drain(step, carry):
        j = step // KINDS
        part = step % KINDS
        for way in (ACROSS, RIGHT, LEFT):

            @pl.when(goes(way, j, part))
            def _():
                remote(way, j, part).wait_send()

        return carry

    lax.fori_loop(0, n * KINDS, drain, 0)


def shards(
    queries, current_keys, current_values, stored_keys, stored_values, remap_table, block_table
):
    tokens, width = queries.shape
    key_width = current_keys.shape[1]
    kv_local = key_width // HEAD_SIZE
    heads = width // HEAD_SIZE
    per_group = heads // kv_local
    my_index = lax.axis_index("seq")
    owners = lax.axis_size("seq")
    positions = (
        jnp.repeat(remap_table, QBLK, axis=1)
        + (jnp.arange(tokens, dtype=jnp.int32) % QBLK)[None, :]
    )
    positions = jnp.stack([positions[2], positions[1], positions[0]])
    half_dim = HEAD_SIZE // 2
    frequency = rope_base ** (-2.0 * jnp.arange(half_dim, dtype=jnp.float32) / HEAD_SIZE)
    angles = positions.astype(jnp.float32)[..., None] * frequency
    cos = jnp.cos(angles)
    sin = jnp.sin(angles)
    cos = jnp.concatenate([cos, cos], -1)
    sin = jnp.concatenate([-sin, sin], -1)
    kv = jnp.stack(
        [
            jnp.stack([stored_keys[:, s, :], stored_values[:, s, :]])
            for s in range(PRIOR_SEGMENTS)
        ]
        + [jnp.stack([current_keys, current_values])]
    )
    rounds = tokens // PAGE_TOKENS // owners
    vmem = pl.BlockSpec(memory_space=pltpu.VMEM)
    attended, raw = pl.pallas_call(
        functools.partial(kernel, owners, kv_local, per_group),
        out_shape=(
            jax.ShapeDtypeStruct((tokens, width), jnp.bfloat16),
            jax.ShapeDtypeStruct((2, owners * rounds, PAGE_TOKENS, key_width), jnp.bfloat16),
        ),
        in_specs=[vmem, vmem, vmem, pl.BlockSpec(memory_space=pl.ANY)],
        out_specs=(vmem, vmem),
        scratch_shapes=[
            pltpu.VMEM((owners, KINDS, 2, tokens, key_width), jnp.bfloat16),
            pltpu.VMEM((KINDS, heads, tokens, HEAD_SIZE), jnp.bfloat16),
            pltpu.VMEM((heads, 1, tokens), jnp.float32),
            pltpu.VMEM((heads, 1, tokens), jnp.float32),
            pltpu.VMEM((heads, HEAD_SIZE, tokens), jnp.float32),
            pltpu.SemaphoreType.DMA,
            pltpu.SemaphoreType.DMA((3, owners, KINDS)),
            pltpu.SemaphoreType.DMA((owners, KINDS)),
        ],
        compiler_params=pltpu.CompilerParams(
            collective_id=0, has_side_effects=True, vmem_limit_bytes=48 * 1024 * 1024
        ),
    )(queries, cos, sin, kv)
    pages_here = owners * rounds
    arranged = (
        raw.reshape(2, pages_here, PAGE_TOKENS, kv_local, HEAD_SIZE)
        .transpose(0, 3, 1, 2, 4)
        .reshape(2, kv_local, pages_here, PAGE_TOKENS * HEAD_SIZE)
    )
    source_index = jnp.arange(owners, dtype=jnp.int32)[:, None]
    round_index = jnp.arange(rounds, dtype=jnp.int32)[None, :]
    block_index = source_index * (tokens // PAGE_TOKENS) + round_index * owners + my_index
    target = block_table[block_index.reshape(-1)]
    paged = jnp.zeros_like(arranged).at[:, :, target].set(arranged)
    return (attended, paged[0], paged[1])


def solution(mesh):
    in_specs = (
        P(("groups", "seq"), "head"),
        P(("groups", "seq"), "head"),
        P(("groups", "seq"), "head"),
        P(("groups", "seq"), None, "head"),
        P(("groups", "seq"), None, "head"),
        P(None, ("groups", "seq")),
        P("groups"),
    )
    out_specs = (
        P(("groups", "seq"), "head"),
        P("head", ("groups", "seq"), None),
        P("head", ("groups", "seq"), None),
    )
    return jax.shard_map(shards, mesh=mesh, in_specs=in_specs, out_specs=out_specs, check_vma=False)
```

```python
import functools
import math

import jax
import jax.numpy as jnp
from jax import lax
from jax.experimental import pallas as pl
from jax.experimental.pallas import tpu as pltpu
from jax.sharding import PartitionSpec as P

HEAD_SIZE = 128
PRIOR_SEGMENTS = 2
PAGE_TOKENS = 16
QBLK = 64
KINDS = PRIOR_SEGMENTS + 1
OWN_PART = PRIOR_SEGMENTS

rope_base = 1000000.0
masked_value = -1e30
MESH = pl.DeviceIdType.MESH
RIGHT, LEFT, ACROSS = 0, 1, 2


def kernel(
    n, kv_local, per_group, q_ref, cos_ref, sin_ref, kv_hbm, out_ref, raw_ref,
    held, turned, top, denom, total, own_sem, send_sem, recv_sem,
):
    me = lax.axis_index("seq")
    partner = me + 1 - 2 * (me % 2)
    tokens = q_ref.shape[0]
    heads = kv_local * per_group
    scale = HEAD_SIZE ** -0.5 * math.log2(math.e)
    has_right = me + 2 < n
    has_left = me - 2 >= 0

    own = pltpu.make_async_copy(kv_hbm, held.at[me], own_sem)
    own.start()
    barrier = pltpu.get_barrier_semaphore()
    pl.semaphore_signal(barrier, inc=1, device_id={"seq": partner}, device_id_type=MESH)

    @pl.when(has_right)
    def _():
        pl.semaphore_signal(barrier, inc=1, device_id={"seq": me + 2}, device_id_type=MESH)

    @pl.when(has_left)
    def _():
        pl.semaphore_signal(barrier, inc=1, device_id={"seq": me - 2}, device_id_type=MESH)

    expected = 1 + has_right.astype(jnp.int32) + has_left.astype(jnp.int32)
    pl.semaphore_wait(barrier, expected)
    own.wait()

    def remote(way, j, part):
        target = (me + 2, me - 2, partner)[way]
        return pltpu.make_async_remote_copy(
            src_ref=held.at[j, part],
            dst_ref=held.at[j, part],
            send_sem=send_sem.at[way, j, part],
            recv_sem=recv_sem.at[j, part],
            device_id={"seq": target},
            device_id_type=MESH,
        )

    def goes(way, j, part):
        mine = (j % 2) == (me % 2)
        stored = part < PRIOR_SEGMENTS
        if way == RIGHT:
            return mine & (j <= me) & has_right
        if way == LEFT:
            return mine & (j >= me) & stored & has_left
        return mine & (stored | (j <= partner))

    def forward(j, part):
        for way in (ACROSS, RIGHT, LEFT):

            @pl.when(goes(way, j, part))
            def _():
                remote(way, j, part).start()

    for part in range(KINDS):
        forward(me, part)

    def turn(part, carry):
        cos = cos_ref[part]
        sin = sin_ref[part]
        for h in range(heads):
            x = q_ref[:, h * HEAD_SIZE : (h + 1) * HEAD_SIZE].astype(jnp.float32)
            y = x * cos + pltpu.roll(x, HEAD_SIZE // 2, 1) * sin
            turned[part, h] = y.T.astype(jnp.bfloat16)
        return carry

    lax.fori_loop(0, KINDS, turn, 0)
    top[...] = jnp.full(top.shape, masked_value, jnp.float32)
    denom[...] = jnp.zeros(denom.shape, jnp.float32)
    total[...] = jnp.zeros(total.shape, jnp.float32)

    def absorb(j, part, causal):
        keys = [held[j, part, 0, :, g * HEAD_SIZE : (g + 1) * HEAD_SIZE] for g in range(kv_local)]
        values = [
            held[j, part, 1, :, g * HEAD_SIZE : (g + 1) * HEAD_SIZE].T for g in range(kv_local)
        ]

        def score(h):
            return jnp.dot(
                keys[h // per_group], turned[part, h], preferred_element_type=jnp.float32
            )

        def add(h, weights, factor):
            total[h] = total[h] * factor + jnp.dot(
                values[h // per_group], weights, preferred_element_type=jnp.float32
            )

        pending = None
        following = score(0)
        for h in range(heads):
            scores = following
            if h + 1 < heads:
                following = score(h + 1)
            if causal:
                key_index = lax.broadcasted_iota(jnp.int32, scores.shape, 0)
                row_index = lax.broadcasted_iota(jnp.int32, scores.shape, 1)
                scores = jnp.where(key_index <= row_index, scores, masked_value)
            old = top[h]
            new = jnp.maximum(old, jnp.max(scores, 0, keepdims=True))
            factor = jnp.exp2((old - new) * scale)
            weights = jnp.exp2((scores - new) * scale)
            top[h] = new
            denom[h] = denom[h] * factor + jnp.sum(weights, 0, keepdims=True)
            if pending is not None:
                add(*pending)
            pending = (h, weights.astype(jnp.bfloat16), factor)
        add(*pending)

    def own_step(part, carry):
        absorb(me, part, False)
        return carry

    lax.fori_loop(0, PRIOR_SEGMENTS, own_step, 0)
    absorb(me, OWN_PART, True)

    def round_step(step, carry):
        distance = step // (4 * KINDS) + 1
        part = (step // 4) % KINDS
        kind = step % 4
        near = distance - kind // 2
        start = jnp.where(kind < 2, me, partner)
        sign = 1 - 2 * (kind % 2)
        j = start - sign * 2 * near
        stored = part < PRIOR_SEGMENTS
        wanted = (j >= 0) & (j < n) & (stored | (j <= me)) & ((near > 0) | (kind % 2 == 0))

        @pl.when(wanted)
        def _():
            remote(RIGHT, j, part).wait_recv()
            forward(j, part)
            absorb(j, part, False)

        return carry

    lax.fori_loop(0, (n // 2) * 4 * KINDS, round_step, 0)

    rounds = tokens // PAGE_TOKENS // n
    last = PRIOR_SEGMENTS - 1

    def page_step(j, carry):
        for r in range(rounds):
            rows = pl.ds(pl.multiple_of((r * n + me) * PAGE_TOKENS, PAGE_TOKENS), PAGE_TOKENS)
            for which in range(2):
                raw_ref[which, j * rounds + r] = held[j, last, which, rows, :]
        return carry

    lax.fori_loop(0, n, page_step, 0)

    for h in range(heads):
        finished = total[h] / denom[h]
        out_ref[:, h * HEAD_SIZE : (h + 1) * HEAD_SIZE] = finished.T.astype(out_ref.dtype)

    def drain(step, carry):
        j = step // KINDS
        part = step % KINDS
        for way in (ACROSS, RIGHT, LEFT):

            @pl.when(goes(way, j, part))
            def _():
                remote(way, j, part).wait_send()

        return carry

    lax.fori_loop(0, n * KINDS, drain, 0)


def shards(
    queries, current_keys, current_values, stored_keys, stored_values, remap_table, block_table
):
    tokens, width = queries.shape
    key_width = current_keys.shape[1]
    kv_local = key_width // HEAD_SIZE
    heads = width // HEAD_SIZE
    per_group = heads // kv_local
    my_index = lax.axis_index("seq")
    owners = lax.axis_size("seq")
    positions = (
        jnp.repeat(remap_table, QBLK, axis=1)
        + (jnp.arange(tokens, dtype=jnp.int32) % QBLK)[None, :]
    )
    positions = jnp.stack([positions[2], positions[1], positions[0]])
    half_dim = HEAD_SIZE // 2
    frequency = rope_base ** (-2.0 * jnp.arange(half_dim, dtype=jnp.float32) / HEAD_SIZE)
    angles = positions.astype(jnp.float32)[..., None] * frequency
    cos = jnp.cos(angles)
    sin = jnp.sin(angles)
    cos = jnp.concatenate([cos, cos], -1)
    sin = jnp.concatenate([-sin, sin], -1)
    kv = jnp.stack(
        [
            jnp.stack([stored_keys[:, s, :], stored_values[:, s, :]])
            for s in range(PRIOR_SEGMENTS)
        ]
        + [jnp.stack([current_keys, current_values])]
    )
    rounds = tokens // PAGE_TOKENS // owners
    vmem = pl.BlockSpec(memory_space=pltpu.VMEM)
    attended, raw = pl.pallas_call(
        functools.partial(kernel, owners, kv_local, per_group),
        out_shape=(
            jax.ShapeDtypeStruct((tokens, width), jnp.bfloat16),
            jax.ShapeDtypeStruct((2, owners * rounds, PAGE_TOKENS, key_width), jnp.bfloat16),
        ),
        in_specs=[vmem, vmem, vmem, pl.BlockSpec(memory_space=pl.ANY)],
        out_specs=(vmem, vmem),
        scratch_shapes=[
            pltpu.VMEM((owners, KINDS, 2, tokens, key_width), jnp.bfloat16),
            pltpu.VMEM((KINDS, heads, HEAD_SIZE, tokens), jnp.bfloat16),
            pltpu.VMEM((heads, 1, tokens), jnp.float32),
            pltpu.VMEM((heads, 1, tokens), jnp.float32),
            pltpu.VMEM((heads, HEAD_SIZE, tokens), jnp.float32),
            pltpu.SemaphoreType.DMA,
            pltpu.SemaphoreType.DMA((3, owners, KINDS)),
            pltpu.SemaphoreType.DMA((owners, KINDS)),
        ],
        compiler_params=pltpu.CompilerParams(
            collective_id=0, has_side_effects=True, vmem_limit_bytes=48 * 1024 * 1024
        ),
    )(queries, cos, sin, kv)
    pages_here = owners * rounds
    arranged = (
        raw.reshape(2, pages_here, PAGE_TOKENS, kv_local, HEAD_SIZE)
        .transpose(0, 3, 1, 2, 4)
        .reshape(2, kv_local, pages_here, PAGE_TOKENS * HEAD_SIZE)
    )
    source_index = jnp.arange(owners, dtype=jnp.int32)[:, None]
    round_index = jnp.arange(rounds, dtype=jnp.int32)[None, :]
    block_index = source_index * (tokens // PAGE_TOKENS) + round_index * owners + my_index
    target = block_table[block_index.reshape(-1)]
    paged = jnp.zeros_like(arranged).at[:, :, target].set(arranged)
    return (attended, paged[0], paged[1])


def solution(mesh):
    in_specs = (
        P(("groups", "seq"), "head"),
        P(("groups", "seq"), "head"),
        P(("groups", "seq"), "head"),
        P(("groups", "seq"), None, "head"),
        P(("groups", "seq"), None, "head"),
        P(None, ("groups", "seq")),
        P("groups"),
    )
    out_specs = (
        P(("groups", "seq"), "head"),
        P("head", ("groups", "seq"), None),
        P("head", ("groups", "seq"), None),
    )
    return jax.shard_map(shards, mesh=mesh, in_specs=in_specs, out_specs=out_specs, check_vma=False)
```

```python
import functools
import math

import jax
import jax.numpy as jnp
from jax import lax
from jax.experimental import pallas as pl
from jax.experimental.pallas import tpu as pltpu
from jax.sharding import PartitionSpec as P

HEAD_SIZE = 128
PRIOR_SEGMENTS = 2
PAGE_TOKENS = 16
QBLK = 64
KINDS = PRIOR_SEGMENTS + 1
OWN_PART = PRIOR_SEGMENTS

rope_base = 1000000.0
masked_value = -1e30
MESH = pl.DeviceIdType.MESH
RIGHT, LEFT, ACROSS = 0, 1, 2


def kernel(
    n, kv_local, per_group, q_hbm, cos_ref, sin_ref, stored_ref, keys_hbm, values_hbm,
    out_ref, raw_ref, q_ref, held, turned, top, denom, total, own_sem, send_sem, recv_sem,
):
    me = lax.axis_index("seq")
    partner = me + 1 - 2 * (me % 2)
    tokens = q_hbm.shape[0]
    heads = kv_local * per_group
    scale = HEAD_SIZE ** -0.5 * math.log2(math.e)
    has_right = me + 2 < n
    has_left = me - 2 >= 0

    own = [
        pltpu.make_async_copy(stored_ref, held.at[me, pl.ds(0, PRIOR_SEGMENTS)], own_sem.at[0]),
        pltpu.make_async_copy(keys_hbm, held.at[me, OWN_PART, 0], own_sem.at[1]),
        pltpu.make_async_copy(values_hbm, held.at[me, OWN_PART, 1], own_sem.at[2]),
        pltpu.make_async_copy(q_hbm, q_ref, own_sem.at[3]),
    ]
    for copy in own:
        copy.start()
    barrier = pltpu.get_barrier_semaphore()
    pl.semaphore_signal(barrier, inc=1, device_id={"seq": partner}, device_id_type=MESH)

    @pl.when(has_right)
    def _():
        pl.semaphore_signal(barrier, inc=1, device_id={"seq": me + 2}, device_id_type=MESH)

    @pl.when(has_left)
    def _():
        pl.semaphore_signal(barrier, inc=1, device_id={"seq": me - 2}, device_id_type=MESH)

    expected = 1 + has_right.astype(jnp.int32) + has_left.astype(jnp.int32)
    pl.semaphore_wait(barrier, expected)
    for copy in own[:3]:
        copy.wait()

    def remote(way, j, part):
        target = (me + 2, me - 2, partner)[way]
        return pltpu.make_async_remote_copy(
            src_ref=held.at[j, part],
            dst_ref=held.at[j, part],
            send_sem=send_sem.at[way, j, part],
            recv_sem=recv_sem.at[j, part],
            device_id={"seq": target},
            device_id_type=MESH,
        )

    def goes(way, j, part):
        mine = (j % 2) == (me % 2)
        stored = part < PRIOR_SEGMENTS
        if way == RIGHT:
            relayed = (j == partner) & (part == 0) & (me + 4 >= n)
            return ((mine & (j <= me)) | relayed) & has_right
        if way == LEFT:
            return mine & (j >= me) & stored & has_left
        relayed = (j == me - 2) & (part == 0) & (me + 2 >= n)
        return mine & (stored | (j <= partner)) & jnp.logical_not(relayed)

    def forward(j, part):
        for way in (ACROSS, RIGHT, LEFT):

            @pl.when(goes(way, j, part))
            def _():
                remote(way, j, part).start()

    for part in range(KINDS):
        forward(me, part)
    own[3].wait()

    def turn(part, carry):
        cos = cos_ref[part]
        sin = sin_ref[part]
        for h in range(heads):
            x = q_ref[:, h * HEAD_SIZE : (h + 1) * HEAD_SIZE].astype(jnp.float32)
            y = x * cos + pltpu.roll(x, HEAD_SIZE // 2, 1) * sin
            turned[part, h] = y.T.astype(jnp.bfloat16)
        return carry

    lax.fori_loop(0, KINDS, turn, 0)
    top[...] = jnp.full(top.shape, masked_value, jnp.float32)
    denom[...] = jnp.zeros(denom.shape, jnp.float32)
    total[...] = jnp.zeros(total.shape, jnp.float32)

    def absorb(j, part, causal):
        keys = [held[j, part, 0, :, g * HEAD_SIZE : (g + 1) * HEAD_SIZE] for g in range(kv_local)]
        values = [
            held[j, part, 1, :, g * HEAD_SIZE : (g + 1) * HEAD_SIZE].T for g in range(kv_local)
        ]

        def score(h):
            return jnp.dot(
                keys[h // per_group], turned[part, h], preferred_element_type=jnp.float32
            )

        def add(h, weights, factor):
            total[h] = total[h] * factor + jnp.dot(
                values[h // per_group], weights, preferred_element_type=jnp.float32
            )

        pending = None
        following = score(0)
        for h in range(heads):
            scores = following
            if h + 1 < heads:
                following = score(h + 1)
            if causal:
                key_index = lax.broadcasted_iota(jnp.int32, scores.shape, 0)
                row_index = lax.broadcasted_iota(jnp.int32, scores.shape, 1)
                scores = jnp.where(key_index <= row_index, scores, masked_value)
            old = top[h]
            new = jnp.maximum(old, jnp.max(scores, 0, keepdims=True))
            factor = jnp.exp2((old - new) * scale)
            weights = jnp.exp2((scores - new) * scale)
            top[h] = new
            denom[h] = denom[h] * factor + jnp.sum(weights, 0, keepdims=True)
            if pending is not None:
                add(*pending)
            pending = (h, weights.astype(jnp.bfloat16), factor)
        add(*pending)

    def own_step(part, carry):
        absorb(me, part, False)
        return carry

    lax.fori_loop(0, PRIOR_SEGMENTS, own_step, 0)
    absorb(me, OWN_PART, True)

    def round_step(step, carry):
        distance = step // (4 * KINDS) + 1
        part = (step // 4) % KINDS
        kind = step % 4
        near = distance - kind // 2
        start = jnp.where(kind < 2, me, partner)
        sign = 1 - 2 * (kind % 2)
        j = start - sign * 2 * near
        stored = part < PRIOR_SEGMENTS
        wanted = (j >= 0) & (j < n) & (stored | (j <= me)) & ((near > 0) | (kind % 2 == 0))

        @pl.when(wanted)
        def _():
            remote(RIGHT, j, part).wait_recv()
            forward(j, part)
            absorb(j, part, False)

        return carry

    lax.fori_loop(0, (n // 2) * 4 * KINDS, round_step, 0)

    rounds = tokens // PAGE_TOKENS // n
    last = PRIOR_SEGMENTS - 1

    def page_step(j, carry):
        for r in range(rounds):
            rows = pl.ds(pl.multiple_of((r * n + me) * PAGE_TOKENS, PAGE_TOKENS), PAGE_TOKENS)
            for which in range(2):
                raw_ref[which, j * rounds + r] = held[j, last, which, rows, :]
        return carry

    lax.fori_loop(0, n, page_step, 0)

    for h in range(heads):
        finished = total[h] / denom[h]
        out_ref[:, h * HEAD_SIZE : (h + 1) * HEAD_SIZE] = finished.T.astype(out_ref.dtype)

    def drain(step, carry):
        j = step // KINDS
        part = step % KINDS
        for way in (ACROSS, RIGHT, LEFT):

            @pl.when(goes(way, j, part))
            def _():
                remote(way, j, part).wait_send()

        return carry

    lax.fori_loop(0, n * KINDS, drain, 0)


def shards(
    queries, current_keys, current_values, stored_keys, stored_values, remap_table, block_table
):
    tokens, width = queries.shape
    key_width = current_keys.shape[1]
    kv_local = key_width // HEAD_SIZE
    heads = width // HEAD_SIZE
    per_group = heads // kv_local
    my_index = lax.axis_index("seq")
    owners = lax.axis_size("seq")
    positions = (
        jnp.repeat(remap_table, QBLK, axis=1)
        + (jnp.arange(tokens, dtype=jnp.int32) % QBLK)[None, :]
    )
    positions = jnp.stack([positions[2], positions[1], positions[0]])
    half_dim = HEAD_SIZE // 2
    frequency = rope_base ** (-2.0 * jnp.arange(half_dim, dtype=jnp.float32) / HEAD_SIZE)
    angles = positions.astype(jnp.float32)[..., None] * frequency
    cos = jnp.cos(angles)
    sin = jnp.sin(angles)
    cos = jnp.concatenate([cos, cos], -1)
    sin = jnp.concatenate([-sin, sin], -1)
    stored = jnp.stack(
        [
            jnp.stack([stored_keys[:, s, :], stored_values[:, s, :]])
            for s in range(PRIOR_SEGMENTS)
        ]
    )
    rounds = tokens // PAGE_TOKENS // owners
    hbm = pl.BlockSpec(memory_space=pltpu.HBM)
    vmem = pl.BlockSpec(memory_space=pltpu.VMEM)
    attended, raw = pl.pallas_call(
        functools.partial(kernel, owners, kv_local, per_group),
        out_shape=(
            jax.ShapeDtypeStruct((tokens, width), jnp.bfloat16),
            jax.ShapeDtypeStruct((2, owners * rounds, PAGE_TOKENS, key_width), jnp.bfloat16),
        ),
        in_specs=[hbm, vmem, vmem, vmem, hbm, hbm],
        out_specs=(vmem, vmem),
        scratch_shapes=[
            pltpu.VMEM((tokens, width), jnp.bfloat16),
            pltpu.VMEM((owners, KINDS, 2, tokens, key_width), jnp.bfloat16),
            pltpu.VMEM((KINDS, heads, HEAD_SIZE, tokens), jnp.bfloat16),
            pltpu.VMEM((heads, 1, tokens), jnp.float32),
            pltpu.VMEM((heads, 1, tokens), jnp.float32),
            pltpu.VMEM((heads, HEAD_SIZE, tokens), jnp.float32),
            pltpu.SemaphoreType.DMA((4,)),
            pltpu.SemaphoreType.DMA((3, owners, KINDS)),
            pltpu.SemaphoreType.DMA((owners, KINDS)),
        ],
        compiler_params=pltpu.CompilerParams(
            collective_id=0, has_side_effects=True, vmem_limit_bytes=48 * 1024 * 1024
        ),
    )(queries, cos, sin, stored, current_keys, current_values)
    pages_here = owners * rounds
    arranged = (
        raw.reshape(2, pages_here, PAGE_TOKENS, kv_local, HEAD_SIZE)
        .transpose(0, 3, 1, 2, 4)
        .reshape(2, kv_local, pages_here, PAGE_TOKENS * HEAD_SIZE)
    )
    source_index = jnp.arange(owners, dtype=jnp.int32)[:, None]
    round_index = jnp.arange(rounds, dtype=jnp.int32)[None, :]
    block_index = source_index * (tokens // PAGE_TOKENS) + round_index * owners + my_index
    target = block_table[block_index.reshape(-1)]
    paged = jnp.zeros_like(arranged).at[:, :, target].set(arranged)
    return (attended, paged[0], paged[1])


def solution(mesh):
    in_specs = (
        P(("groups", "seq"), "head"),
        P(("groups", "seq"), "head"),
        P(("groups", "seq"), "head"),
        P(("groups", "seq"), None, "head"),
        P(("groups", "seq"), None, "head"),
        P(None, ("groups", "seq")),
        P("groups"),
    )
    out_specs = (
        P(("groups", "seq"), "head"),
        P("head", ("groups", "seq"), None),
        P("head", ("groups", "seq"), None),
    )
    return jax.shard_map(shards, mesh=mesh, in_specs=in_specs, out_specs=out_specs, check_vma=False)
```
